32 devices in a mesh: groups: 2 (over y), kvb: 4 (over z), tp: 4 (over x, core).
Axes of the slice: x: 2, y: 2, z: 4, core: 2. Of those that a mesh axis runs over, the one named last changes fastest.
Arguments:
- residual: bfloat16 [32, 8192], P(('groups', 'kvb')), parts along dimension 0, may hold values from -3 to 3
- queries: bfloat16 [32, 8192], P(('groups', 'kvb'), 'tp'), parts along dimension 0, may hold values from -60 to 60
- new_kv: bfloat16 [32, 2048], P(('groups', 'kvb')), parts along dimension 0, may hold values from -6 to 6
- kv_cache: bfloat16 [2048, 16, 2048], P(('groups', 'kvb', 'tp')), parts along dimension 0, may hold values from -6 to 6
- lengths: int32 [32], P('groups'), parts along dimension 0, may hold values from 1 to 2048, as said below
- slot_seq: int32 [2048], P(('groups', 'kvb', 'tp')), parts along dimension 0, may hold values from 0 to 15, as said below
- slot_block: int32 [2048], P(('groups', 'kvb', 'tp')), parts along dimension 0, may hold values from 0 to 127, as said below
- block_counts: int32 [32], P(('groups', 'kvb', 'tp')), parts along dimension 0, may hold values from 16 to 64, as said below
- out_weight: bfloat16 [8192, 8192], P('tp'), may hold values from -0.5 to 0.5
- norm_gain: bfloat16 [8192], P('tp'), may hold values from 0.099609375 to 1.8984375
Outputs:
- stream: bfloat16 [32, 8192], P(('groups', 'kvb'), 'tp'), parts along dimension 0
- normed: bfloat16 [32, 8192], P(('groups', 'kvb'), 'tp'), parts along dimension 0
The draws below stay inside these ranges and needn't reach their ends.
There are 2 independent parts, one for each index of `groups`. The reference program is written for one: setup_inputs(seed, part) draws one part's arguments, and reference() takes and returns one part's arrays. A program takes and returns all parts, laid end to end along the dimension named above; an argument that names none is the same for every part. Nothing has to cross between parts.
Inputs may be any that keep to these rules, and one draw needn't show every extreme that they name: `block_counts`: slots below a device's count hold cache blocks, those at or beyond it none; at least one device's count is 64. `slot_seq`: each pair of a sequence s and a block b below ceil(lengths[s] / 16) sits in exactly one live slot of the group. `slot_block`: some sequence has exactly 128 blocks; none has more. `lengths`: some sequence has exactly 16 * (128) tokens.
All inputs are finite; a program needn't handle non-finite values.
Results may differ from the reference program's by a relative error of at most 0.006.
Values may be sent and summed in bfloat16 or wider, within the bound.
A program may use at most 64 MiB of HBM per device.

```python
import jax
import jax.numpy as jnp
from jax import lax

D = 8192
QH = 64
KVH = 8
HD = 128
BLK = 16
POOL = 64
GROUP = 16
SEQS = 16
SLOTS = 1024


def layout(key):
    base = jax.random.fold_in(key, 7)
    streams = jax.random.split(base, 8)
    floor_count = max(POOL // 4, 1)
    divider = jax.random.randint(streams[0], (GROUP,), 1, 5)
    jitter = jax.random.randint(streams[1], (GROUP,), 0, 4)
    counts = jnp.maximum(POOL // divider - jitter, floor_count)
    fullest = jax.random.randint(streams[2], (), 0, GROUP)
    counts = jnp.where(jnp.arange(GROUP) == fullest, POOL, counts).astype(jnp.int32)
    used = (jnp.arange(POOL)[None, :] < counts[:, None]).reshape(-1)
    priority = jax.random.permutation(streams[3], SLOTS).astype(jnp.int32)
    priority = jnp.where(used, priority, priority + SLOTS)
    order = jnp.argsort(priority)
    rank = jnp.argsort(order).astype(jnp.int32)
    total_used = jnp.sum(counts).astype(jnp.int32)
    most_blocks = SLOTS // 8
    longest = jax.random.randint(streams[7], (), 0, SEQS)
    seq_ids = jnp.arange(SEQS, dtype=jnp.int32)
    is_long = seq_ids == longest
    remaining = total_used - most_blocks
    seq_weight = jnp.where(is_long, 0, jax.random.randint(streams[4], (SEQS,), 1, 64)).astype(jnp.int32)
    cumulative = jnp.cumsum(seq_weight).astype(jnp.int32)
    share_ends = (remaining - (SEQS - 1)) * cumulative // cumulative[-1]
    share_starts = jnp.concatenate([jnp.zeros((1,), jnp.int32), share_ends[:-1]])
    proposed = jnp.where(is_long, 0, share_ends - share_starts + 1)
    capped = jnp.minimum(proposed, most_blocks)
    deficit = remaining - jnp.sum(capped)
    headroom = jnp.where(is_long, 0, most_blocks - capped)
    before = jnp.cumsum(headroom) - headroom
    extra = jnp.clip(deficit - before, 0, headroom)
    blocks = jnp.where(is_long, most_blocks, capped + extra).astype(jnp.int32)
    ends = jnp.cumsum(blocks).astype(jnp.int32)
    starts = (ends - blocks).astype(jnp.int32)
    owner = jnp.sum((rank[:, None] >= ends[None, :]).astype(jnp.int32), axis=1)
    owner = jnp.minimum(owner, SEQS - 1)
    start_of = jnp.take(starts, owner)
    filler = jax.random.randint(streams[5], (SLOTS,), 0, SEQS)
    seq_table = jnp.where(used, owner, filler).astype(jnp.int32)
    block_table = jnp.where(used, rank - start_of, 0).astype(jnp.int32)
    dropped = jnp.where(is_long, 0, jax.random.randint(streams[6], (SEQS,), 0, BLK))
    seq_lengths = (BLK * blocks - dropped).astype(jnp.int32)
    return (seq_lengths, seq_table, block_table, counts)


def draw_lengths(key, part):
    return layout(key)[0]


def draw_slot_seq(key, part):
    return layout(key)[1]


def draw_slot_block(key, part):
    return layout(key)[2]


def draw_block_counts(key, part):
    return layout(key)[3]


def draw_kv_cache(key, part):
    cache = jax.random.normal(jax.random.fold_in(key, 29), (SLOTS, BLK, 2 * KVH * HD), jnp.float32)
    cache = jnp.clip(cache, -6.0, 6.0)
    return cache.astype(jnp.bfloat16)


def draw_queries(key, part):
    values = jax.random.normal(jax.random.fold_in(key, 41), (SEQS, QH * HD), jnp.float32)
    values = jnp.clip(values, -6.0, 6.0)
    return values.astype(jnp.bfloat16)


def levels(key, extent, shards, least, high):
    def one(dim, blocks):
        steps = jax.random.uniform(jax.random.fold_in(jax.random.fold_in(key, 6), dim), (blocks,), jnp.float32, least / len(shards), high / len(shards))
        return jnp.repeat(jnp.exp(steps), extent[dim] // blocks).reshape((-1,) + (1,) * (len(extent) - dim - 1))

    loudness = one(*shards[0])
    for cut in shards[1:]:
        loudness = loudness * one(*cut)
    return loudness


def noise(own_key, extent, scale, reach, shards=(), kind=jnp.bfloat16):
    drawn = jax.random.normal(own_key, extent, jnp.float32) * scale
    if len(shards) > 0:
        drawn = levels(own_key, extent, shards, -0.22, 0.18) * drawn
    return jnp.clip(drawn, min=-reach, max=reach).astype(kind)


def setup_inputs(seed: int = 0, part: int = 0) -> dict:
    streams_of = jax.random.split(jax.random.key(seed), 11)
    own_keys = jax.random.split(jax.random.fold_in(streams_of[10], part), 11)
    residual = noise(own_keys[0], (SEQS, D), 0.5, 3.0, ((0, 4),))
    queries = draw_queries(jax.random.fold_in(jax.random.fold_in(streams_of[10], part), 71), part)
    new_kv = noise(own_keys[2], (SEQS, 2 * KVH * HD), 1.0, 6.0, ((0, 4),))
    kv_cache = draw_kv_cache(jax.random.fold_in(jax.random.fold_in(streams_of[10], part), 71), part)
    lengths = draw_lengths(jax.random.fold_in(jax.random.fold_in(streams_of[10], part), 71), part)
    slot_seq = draw_slot_seq(jax.random.fold_in(jax.random.fold_in(streams_of[10], part), 71), part)
    slot_block = draw_slot_block(jax.random.fold_in(jax.random.fold_in(streams_of[10], part), 71), part)
    block_counts = draw_block_counts(jax.random.fold_in(jax.random.fold_in(streams_of[10], part), 71), part)
    out_weight = noise(streams_of[8], (QH * HD, D), HD ** -0.5, 0.5, ((0, 4),))
    norm_gain = jnp.clip(1.0 + 0.18 * jax.random.normal(streams_of[9], (D,), jnp.float32), 0.099609375, 1.8984375).astype(jnp.bfloat16)
    return dict(residual=residual, queries=queries, new_kv=new_kv, kv_cache=kv_cache, lengths=lengths, slot_seq=slot_seq, slot_block=slot_block, block_counts=block_counts, out_weight=out_weight, norm_gain=norm_gain)


NEGATIVE = -1e+30
EPSILON = 1e-06

def pool_partial(grouped, cache_pool, seq_pool, block_pool, live_count, lengths):
    pool_size = cache_pool.shape[0]
    key_rows = cache_pool[:, :, :KVH * HD].reshape(pool_size * BLK, KVH, HD).astype(jnp.float32)
    value_rows = cache_pool[:, :, KVH * HD:].reshape(pool_size * BLK, KVH, HD).astype(jnp.float32)
    token_seq = jnp.repeat(seq_pool, BLK)
    position = (block_pool[:, None] * BLK + jnp.arange(BLK, dtype=jnp.int32)[None, :]).reshape(-1)
    slot_live = jnp.repeat(jnp.arange(pool_size, dtype=jnp.int32) < live_count, BLK)
    member = token_seq[None, :] == jnp.arange(SEQS, dtype=jnp.int32)[:, None]
    length_of = lax.optimization_barrier(jnp.sum(jnp.where(member, lengths[:, None], 0), axis=0))
    live = member & (position < length_of)[None, :] & slot_live[None, :]
    mask = live[:, None, None, :]
    scores = jnp.einsum('sgqd,ngd->sgqn', grouped.astype(jnp.float32), key_rows) * HD ** (-0.5)
    peak_now = lax.optimization_barrier(jnp.max(jnp.where(mask, scores, NEGATIVE), axis=-1))
    weights = jnp.where(mask, jnp.exp(scores - peak_now[..., None]), 0.0)
    weight_sum = lax.optimization_barrier(jnp.sum(weights, axis=-1))
    rounded = weights.astype(jnp.bfloat16).astype(jnp.float32)
    partial_rows = jnp.einsum('sgqn,ngd->sgqd', rounded, value_rows)
    return (peak_now, weight_sum, partial_rows)

def reference(residual, queries, new_kv, kv_cache, lengths, slot_seq, slot_block, block_counts, out_weight, norm_gain):
    grouped = queries.reshape(SEQS, KVH, QH // KVH, HD)
    cache_groups = kv_cache.reshape(GROUP, POOL, BLK, 2 * KVH * HD)
    seq_groups = slot_seq.reshape(GROUP, POOL)
    block_groups = slot_block.reshape(GROUP, POOL)

    def one_pool(pieces):
        return pool_partial(grouped, pieces[0], pieces[1], pieces[2], pieces[3], lengths)
    peaks, sums, partials = lax.map(one_pool, (cache_groups, seq_groups, block_groups, block_counts))
    new_keys = new_kv[:, :KVH * HD].reshape(SEQS, KVH, HD).astype(jnp.float32)
    new_values = new_kv[:, KVH * HD:].reshape(SEQS, KVH, HD).astype(jnp.float32)
    fresh = jnp.einsum('sgqd,sgd->sgq', grouped.astype(jnp.float32), new_keys) * HD ** (-0.5)
    overall = jnp.maximum(lax.optimization_barrier(jnp.max(peaks, axis=0)), fresh)
    scaling = jnp.exp(peaks - overall[None])
    fresh_weight = jnp.exp(fresh - overall)
    denominator = lax.optimization_barrier(jnp.sum(scaling * sums, axis=0)) + fresh_weight
    numerator = lax.optimization_barrier(jnp.sum(scaling[..., None] * partials, axis=0)) + fresh_weight[..., None] * new_values[:, :, None, :]
    attended = (numerator / denominator[..., None]).reshape(SEQS, QH * HD).astype(jnp.bfloat16)
    projected = jnp.dot(attended, out_weight, preferred_element_type=jnp.float32)
    stream = (residual.astype(jnp.float32) + projected).astype(jnp.bfloat16)
    stream_wide = lax.optimization_barrier(stream).astype(jnp.float32)
    mean_square = lax.optimization_barrier(jnp.mean(stream_wide * stream_wide, axis=1, keepdims=True))
    normed = (stream_wide * lax.rsqrt(mean_square + EPSILON) * norm_gain.astype(jnp.float32)).astype(jnp.bfloat16)
    return (stream, normed)
```

```python
import math

import jax
import jax.numpy as jnp
from jax import lax
from jax.experimental import pallas as pl
from jax.experimental.pallas import tpu as pltpu
from jax.sharding import PartitionSpec as P

QH = 64
KVH = 8
HD = 128
BLK = 16
GROUP_HEADS = QH // KVH

NEGATIVE = -1e30
EPSILON = 1e-06
LANES = 128
TOKEN_LOG2 = math.log2(math.e) * HD ** (-0.5)
MESH = pl.DeviceIdType.MESH


def kernel(
    nz,
    nt,
    seq_rep,
    local_heads,
    counts_ref,
    lengths_hbm,
    slot_seq_hbm,
    slot_block_hbm,
    residual_hbm,
    queries_hbm,
    new_kv_hbm,
    gain_hbm,
    cache_ref,
    weight_ref,
    stream_ref,
    factor_ref,
    lengths_ref,
    slot_seq_ref,
    slot_block_ref,
    residual_ref,
    queries_ref,
    new_kv_ref,
    gain_ref,
    wide_gain,
    cache_buf,
    weight_buf,
    bias_buf,
    row_buf,
    new_buf,
    q_all,
    part_tp,
    stat_tp,
    part_send,
    stat_send,
    z_send,
    z_stat_send,
    z_part,
    z_stat,
    lhs_buf,
    proj_sum,
    proj_send,
    proj_recv,
    ss_send,
    ss_recv,
    input_sem,
    cache_sem,
    weight_sem,
    qz_send,
    qz_recv,
    qt_send,
    qt_recv,
    pt_send,
    pt_recv,
    st_send,
    st_recv,
    zp_send,
    zp_recv,
    zs_send,
    zs_recv,
    rs_send,
    rs_recv,
    sq_send,
    sq_recv,
):
    z = lax.axis_index("kvb")
    t = lax.axis_index("tp")
    kv_local = max(1, local_heads // GROUP_HEADS)
    per_kv = local_heads // kv_local
    sub = per_kv * seq_rep
    rows = nz * sub
    tokens = cache_buf.shape[0]
    slots = slot_seq_ref.shape[1]
    width = stream_ref.shape[1]
    fast = 2 if nt % 2 == 0 else 1
    slow = nt // fast

    def tp_to(j):
        return lax.rem(t // fast + j // fast, slow) * fast + lax.rem(t % fast + j % fast, fast)

    def tp_from(j):
        back = (slow - j // fast) % slow
        back_fast = (fast - j % fast) % fast
        return lax.rem(t // fast + back, slow) * fast + lax.rem(t % fast + back_fast, fast)

    def z_to(a):
        return lax.rem(z + a, nz)

    def z_back(a):
        return lax.rem(z + (nz - a), nz)

    far_first = sorted(range(1, nt), key=lambda j: (j < fast, j))

    barrier = pltpu.get_barrier_semaphore()
    for a in range(1, nz):
        pl.semaphore_signal(barrier, inc=1, device_id={"kvb": z_to(a)}, device_id_type=MESH)
    for j in range(1, nt):
        pl.semaphore_signal(barrier, inc=1, device_id={"tp": tp_to(j)}, device_id_type=MESH)

    own = pl.ds(pl.multiple_of(t * width, LANES), width)
    inputs = [
        pltpu.make_async_copy(src, dst, input_sem.at[i])
        for i, (src, dst) in enumerate(
            (
                (queries_hbm, queries_ref),
                (slot_seq_hbm, slot_seq_ref),
                (slot_block_hbm, slot_block_ref),
                (new_kv_hbm, new_kv_ref),
                (residual_hbm.at[:, own], residual_ref),
                (gain_hbm, gain_ref),
                (lengths_hbm, lengths_ref),
            )
        )
    ]
    for copy in inputs:
        copy.start()
    cache_copy = pltpu.make_async_copy(cache_ref, cache_buf, cache_sem)
    cache_copy.start()
    inputs[0].wait()

    wide_q = queries_ref[...].astype(jnp.float32)
    for k in range(kv_local):
        for q in range(per_kv):
            head = k * per_kv + q
            row_buf[k, q * seq_rep : (q + 1) * seq_rep, :] = wide_q[:, head * HD : (head + 1) * HD]
    for k in range(kv_local):
        q_all[0, 0, k] = row_buf[k].astype(jnp.bfloat16)
    with jax.named_scope("barrier_wait"):
        pl.semaphore_wait(barrier, nz - 1 + nt - 1)

    pending = []

    def remote(src, dst, send, recv, target):
        copy = pltpu.make_async_remote_copy(
            src_ref=src,
            dst_ref=dst,
            send_sem=send,
            recv_sem=recv,
            device_id=target,
            device_id_type=MESH,
        )
        copy.start()
        pending.append(copy)
        return copy

    z_order = sorted(range(1, nz), key=lambda a: min(a, nz - a))
    q_from_z = {}
    for a in reversed(z_order):
        q_from_z[a] = remote(
            q_all.at[0, 0], q_all.at[0, a], qz_send.at[a], qz_recv.at[a], {"kvb": z_to(a)}
        )
    q_from_tp = {}

    def relayed(j):
        return fast == 2 and j > 2 and j % 2 == 1

    def relay(j):
        for a in [0] + z_order:
            with jax.named_scope(f"q_relay_wait{j}"):
                q_from_tp[a, j].wait_recv()
            q_from_tp[a, j + 1] = remote(
                q_all.at[j, a],
                q_all.at[j + 1, a],
                qt_send.at[a, j + 1],
                qt_recv.at[a, j + 1],
                {"tp": tp_to(1)},
            )

    def forward(a):
        for j in far_first:
            if relayed(j):
                continue
            q_from_tp[a, j] = remote(
                q_all.at[0, a],
                q_all.at[j, a],
                qt_send.at[a, j],
                qt_recv.at[a, j],
                {"tp": tp_to(j)},
            )

    forward(0)

    depth = weight_buf.shape[0] // kv_local
    pieces = 4
    weight_copies = []
    for i in range(kv_local * pieces):
        part_rows = pl.ds(i * (depth // pieces), depth // pieces)
        weight_copies.append(
            pltpu.make_async_copy(
                weight_ref.at[part_rows, :], weight_buf.at[part_rows, :], weight_sem.at[i]
            )
        )
        weight_copies[i].start()
    for copy in inputs[1:]:
        copy.wait()

    row_id = lax.broadcasted_iota(jnp.int32, (rows, slots), 0)
    slot_id = lax.broadcasted_iota(jnp.int32, (rows, slots), 1)
    row_seq = lax.rem(z + nz - row_id // sub, nz) * seq_rep + lax.rem(row_id, seq_rep)
    row_len = jnp.zeros((rows, slots), jnp.int32)
    for s in range(nz * seq_rep):
        row_len = jnp.where(row_seq == s, lengths_ref[s], row_len)
    held = (row_seq == slot_seq_ref[...]) & (slot_id < counts_ref[0])
    limit = jnp.where(held, jnp.clip(row_len - BLK * slot_block_ref[...], 0, BLK), 0)
    token_slot = lax.broadcasted_iota(jnp.int32, (slots, tokens), 1) // BLK
    spread = (token_slot == lax.broadcasted_iota(jnp.int32, (slots, tokens), 0)).astype(jnp.float32)
    reach = jnp.dot(
        limit.astype(jnp.float32).astype(jnp.bfloat16),
        spread.astype(jnp.bfloat16),
        preferred_element_type=jnp.float32,
    )
    offset = lax.rem(lax.broadcasted_iota(jnp.int32, (rows, tokens), 1), BLK).astype(jnp.float32)
    bias_buf[...] = jnp.where(offset < reach, 0.0, NEGATIVE)

    own_kv = t * local_heads // GROUP_HEADS
    fresh = []
    for k in range(kv_local):
        for part in range(2):
            at = pl.multiple_of((part * KVH + own_kv + k) * HD, LANES)
            piece = new_kv_ref[:, pl.ds(at, HD)].astype(jnp.float32)
            for q in range(per_kv):
                new_buf[k, part, q * seq_rep : (q + 1) * seq_rep, :] = piece
        fresh.append(jnp.sum(row_buf[k] * new_buf[k, 0], axis=1, keepdims=True) * TOKEN_LOG2)
    lhs_buf[...] = jnp.zeros_like(lhs_buf)
    gain = gain_ref[...].astype(jnp.float32).reshape(1, width)
    wide_gain[...] = jnp.broadcast_to(gain, wide_gain.shape)

    for a in z_order:
        with jax.named_scope(f"q_z_wait{a}"):
            q_from_z[a].wait_recv()
        forward(a)

    with jax.named_scope("cache_wait"):
        cache_copy.wait()
    lane = lax.broadcasted_iota(jnp.int32, (rows, LANES), 1)
    copies = {}

    def attend(j, k):
        first_kv = tp_from(j) * local_heads // GROUP_HEADS
        key_at = pl.multiple_of((first_kv + k) * HD, LANES)
        value_at = pl.multiple_of((KVH + first_kv + k) * HD, LANES)
        q_rows = q_all[j, :, k].reshape(rows, HD)
        scores = lax.dot_general(
            q_rows,
            cache_buf[:, pl.ds(key_at, HD)],
            (((1,), (1,)), ((), ())),
            preferred_element_type=jnp.float32,
        )
        scores = scores * TOKEN_LOG2 + bias_buf[...]
        peak = jnp.max(scores, axis=1, keepdims=True)
        weights = jnp.exp2(scores - jnp.maximum(peak, 0.1 * NEGATIVE))
        total = jnp.sum(weights, axis=1, keepdims=True)
        partial = jnp.dot(
            weights.astype(jnp.bfloat16),
            cache_buf[:, pl.ds(value_at, HD)],
            preferred_element_type=jnp.float32,
        ).astype(jnp.bfloat16)
        tile = jnp.where(lane == 0, peak, total).T[:8]
        if j == 0:
            part_tp[0, k] = partial
            stat_tp[0, k] = tile
            return
        part_send[j, k] = partial
        stat_send[j, k] = tile
        target = {"tp": tp_from(j)}
        copies[j, k] = (
            remote(
                stat_send.at[j, k],
                stat_tp.at[j, k],
                st_send.at[j, k],
                st_recv.at[j, k],
                target,
            ),
            remote(
                part_send.at[j, k],
                part_tp.at[j, k],
                pt_send.at[j, k],
                pt_recv.at[j, k],
                target,
            ),
        )

    for k in range(kv_local):
        attend(0, k)
    arrived = set()
    for k in range(kv_local):
        for j in far_first if k == kv_local - 1 else range(1, nt):
            if j not in arrived and relayed(j + 1):
                arrived.add(j)
                relay(j)
            elif j not in arrived:
                arrived.add(j)
                with jax.named_scope(f"q_tp_wait{j}"):
                    for a in range(nz):
                        q_from_tp[a, j].wait_recv()
            attend(j, k)

    def columns_of(pieces):
        height = -(-len(pieces) // 8) * 8
        index = lax.broadcasted_iota(jnp.int32, (height, rows), 0)
        tile = jnp.zeros((height, rows), jnp.float32)
        for i, piece in enumerate(pieces):
            tile = jnp.where(index == i, piece, tile)
        return tile.T

    from_z = {}
    for k in range(kv_local):
        with jax.named_scope(f"part_wait{k}"):
            for j in range(1, nt):
                for copy in copies[j, k]:
                    copy.wait_recv()
        peaks = [stat_tp[j, k, 0:1, :] for j in range(nt)]
        top = peaks[0]
        for piece in peaks[1:]:
            top = jnp.maximum(top, piece)
        scale = [jnp.exp2(piece - top) for piece in peaks]
        total = scale[0] * stat_tp[0, k, 1:2, :]
        for j in range(1, nt):
            total += scale[j] * stat_tp[j, k, 1:2, :]
        spread_scale = columns_of(scale)
        joined = spread_scale[:, 0:1] * part_tp[0, k].astype(jnp.float32)
        for j in range(1, nt):
            joined += spread_scale[:, j : j + 1] * part_tp[j, k].astype(jnp.float32)
        joined = joined.astype(jnp.bfloat16)
        index = lax.broadcasted_iota(jnp.int32, (8, rows), 0)
        tile = jnp.where(index == 0, top, total)
        z_stat_send[k] = tile
        z_stat[0, k] = tile
        z_part[0, k] = joined[:sub]
        for a in range(1, nz):
            z_send[a, k] = joined[a * sub : (a + 1) * sub]
        for a in reversed(z_order):
            target = {"kvb": z_back(a)}
            from_z[a, k] = (
                remote(
                    z_stat_send.at[k],
                    z_stat.at[a, k],
                    zs_send.at[a, k],
                    zs_recv.at[a, k],
                    target,
                ),
                remote(
                    z_send.at[a, k],
                    z_part.at[a, k],
                    zp_send.at[a, k],
                    zp_recv.at[a, k],
                    target,
                ),
            )

    step = width
    reduced = {}
    for k in range(kv_local):
        with jax.named_scope(f"z_wait{k}"):
            for a in z_order:
                for copy in from_z[a, k]:
                    copy.wait_recv()
        spread_stat = columns_of([z_stat[a, k, i : i + 1, :] for a in range(nz) for i in range(2)])
        peaks = [spread_stat[a * sub : (a + 1) * sub, 2 * a : 2 * a + 1] for a in range(nz)]
        sums = [spread_stat[a * sub : (a + 1) * sub, 2 * a + 1 : 2 * a + 2] for a in range(nz)]
        top = fresh[k]
        for piece in peaks:
            top = jnp.maximum(top, piece)
        denominator = jnp.exp2(fresh[k] - top)
        numerator = denominator * new_buf[k, 1]
        for a in range(nz):
            scale = jnp.exp2(peaks[a] - top)
            denominator += scale * sums[a]
            numerator += scale * z_part[a, k].astype(jnp.float32)
        row_buf[k] = numerator / denominator
        for q in range(per_kv):
            lhs_buf[k, 0:seq_rep, q * HD : (q + 1) * HD] = row_buf[
                k, q * seq_rep : (q + 1) * seq_rep, :
            ]
        attended = lhs_buf[k].astype(jnp.bfloat16)
        with jax.named_scope(f"weight_wait{k}"):
            for copy in weight_copies[k * pieces : (k + 1) * pieces]:
                copy.wait()
        for j in far_first + [0]:
            column = tp_to(j) * width

            def column_step(i, carry, j=j, k=k, column=column, attended=attended):
                at = pl.ds(pl.multiple_of(i * step, LANES), step)
                source = pl.ds(pl.multiple_of(column + i * step, LANES), step)
                got = jnp.dot(
                    attended,
                    weight_buf[k * depth : (k + 1) * depth, source],
                    preferred_element_type=jnp.float32,
                )[:seq_rep]
                if k > 0:
                    got += proj_sum[j, :, at]
                if j > 0 and k == kv_local - 1:
                    proj_send[j, :, at] = got.astype(jnp.bfloat16)
                else:
                    proj_sum[j, :, at] = got
                return carry

            lax.fori_loop(0, width // step, column_step, 0)
            if j > 0 and k == kv_local - 1:
                reduced[j] = remote(
                    proj_send.at[j],
                    proj_recv.at[j],
                    rs_send.at[j],
                    rs_recv.at[j],
                    {"tp": tp_to(j)},
                )
    summed = residual_ref[...].astype(jnp.float32) + proj_sum[0]
    for copy in pending[: -len(reduced)]:
        copy.wait_send()
    del pending[: -len(reduced)]
    with jax.named_scope("sum_wait"):
        for j in far_first:
            reduced[j].wait_recv()
    for j in far_first:
        summed += proj_recv[j].astype(jnp.float32)
    stream = summed.astype(jnp.bfloat16)
    stream_wide = stream.astype(jnp.float32)
    stream_ref[...] = stream_wide
    square = jnp.sum(stream_wide * stream_wide, axis=1, keepdims=True)
    ss_send[...] = jnp.broadcast_to(square, ss_send.shape)
    squares = [
        remote(ss_send, ss_recv.at[j], sq_send.at[j], sq_recv.at[j], {"tp": tp_to(j)})
        for j in far_first
    ]
    with jax.named_scope("square_wait"):
        for copy in squares:
            copy.wait_recv()
    for j in range(1, nt):
        square += ss_recv[j][:, 0:1]
    mean_square = square * (1.0 / (width * nt))
    factor_ref[...] = lax.rsqrt(mean_square + EPSILON) * wide_gain[...]
    for copy in pending:
        copy.wait_send()


def on_device(
    residual,
    queries,
    new_kv,
    kv_cache,
    lengths,
    slot_seq,
    slot_block,
    block_counts,
    out_weight,
    norm_gain,
):
    nt = lax.axis_size("tp")
    nz = lax.axis_size("kvb")
    seq_rep = residual.shape[0]
    local_heads = queries.shape[1] // HD
    kv_local = max(1, local_heads // GROUP_HEADS)
    sub = local_heads // kv_local * seq_rep
    rows = nz * sub
    slots = kv_cache.shape[0]
    tokens = slots * BLK
    width = norm_gain.shape[0]
    depth = out_weight.shape[0]
    bf16, f32 = jnp.bfloat16, jnp.float32
    dma = pltpu.SemaphoreType.DMA
    smem = pl.BlockSpec(memory_space=pltpu.SMEM)
    vmem = pl.BlockSpec(memory_space=pltpu.VMEM)
    hbm = pl.BlockSpec(memory_space=pl.ANY)

    def body(*refs):
        kernel(nz, nt, seq_rep, local_heads, *refs)

    stream, factor = pl.pallas_call(
        body,
        out_shape=(
            jax.ShapeDtypeStruct((seq_rep, width), f32),
            jax.ShapeDtypeStruct((seq_rep, width), f32),
        ),
        in_specs=[smem] + [hbm] * 9,
        out_specs=(vmem, vmem),
        scratch_shapes=[
            pltpu.SMEM(lengths.shape, jnp.int32),
            pltpu.VMEM((1, slots), jnp.int32),
            pltpu.VMEM((1, slots), jnp.int32),
            pltpu.VMEM((seq_rep, width), bf16),
            pltpu.VMEM(queries.shape, bf16),
            pltpu.VMEM(new_kv.shape, bf16),
            pltpu.VMEM((width,), bf16),
            pltpu.VMEM((seq_rep, width), f32),
            pltpu.VMEM((tokens, kv_cache.shape[2]), bf16),
            pltpu.VMEM(out_weight.shape, bf16),
            pltpu.VMEM((rows, tokens), f32),
            pltpu.VMEM((kv_local, sub, HD), f32),
            pltpu.VMEM((kv_local, 2, sub, HD), f32),
            pltpu.VMEM((nt, nz, kv_local, sub, HD), bf16),
            pltpu.VMEM((nt, kv_local, rows, HD), bf16),
            pltpu.VMEM((nt, kv_local, 8, rows), f32),
            pltpu.VMEM((nt, kv_local, rows, HD), bf16),
            pltpu.VMEM((nt, kv_local, 8, rows), f32),
            pltpu.VMEM((nz, kv_local, sub, HD), bf16),
            pltpu.VMEM((kv_local, 8, rows), f32),
            pltpu.VMEM((nz, kv_local, sub, HD), bf16),
            pltpu.VMEM((nz, kv_local, 8, rows), f32),
            pltpu.VMEM((kv_local, 16, depth // kv_local), f32),
            pltpu.VMEM((nt, seq_rep, width), f32),
            pltpu.VMEM((nt, seq_rep, width), bf16),
            pltpu.VMEM((nt, seq_rep, width), bf16),
            pltpu.VMEM((seq_rep, LANES), f32),
            pltpu.VMEM((nt, seq_rep, LANES), f32),
            dma((7,)),
            dma,
            dma((kv_local * 4,)),
            dma((nz,)),
            dma((nz,)),
            dma((nz, nt)),
            dma((nz, nt)),
            dma((nt, kv_local)),
            dma((nt, kv_local)),
            dma((nt, kv_local)),
            dma((nt, kv_local)),
            dma((nz, kv_local)),
            dma((nz, kv_local)),
            dma((nz, kv_local)),
            dma((nz, kv_local)),
            dma((nt,)),
            dma((nt,)),
            dma((nt,)),
            dma((nt,)),
        ],
        compiler_params=pltpu.CompilerParams(
            collective_id=0, has_side_effects=True, vmem_limit_bytes=46 * 1024 * 1024
        ),
    )(
        block_counts,
        *(
            pltpu.with_memory_space_constraint(operand, pltpu.HBM)
            for operand in (
                lengths,
                slot_seq.reshape(1, slots),
                slot_block.reshape(1, slots),
                residual,
                queries,
                new_kv,
                norm_gain,
                kv_cache.reshape(tokens, kv_cache.shape[2]),
                out_weight,
            )
        )
    )
    return (stream.astype(bf16), (stream * factor).astype(bf16))


def solution(mesh):
    placed = (
        P(("groups", "kvb"), None),
        P(("groups", "kvb"), "tp"),
        P(("groups", "kvb"), None),
        P(("groups", "kvb", "tp"), None, None),
        P("groups"),
        P(("groups", "kvb", "tp")),
        P(("groups", "kvb", "tp")),
        P(("groups", "kvb", "tp")),
        P("tp", None),
        P("tp"),
    )
    return jax.shard_map(
        on_device,
        mesh=mesh,
        in_specs=placed,
        out_specs=(P(("groups", "kvb"), "tp"), P(("groups", "kvb"), "tp")),
        check_vma=False,
    )
```

```python
import math

import jax
import jax.numpy as jnp
from jax import lax
from jax.experimental import pallas as pl
from jax.experimental.pallas import tpu as pltpu
from jax.sharding import PartitionSpec as P

QH = 64
KVH = 8
HD = 128
BLK = 16
GROUP_HEADS = QH // KVH

NEGATIVE = -1e30
EPSILON = 1e-06
LANES = 128
CORES = 2
TOKEN_LOG2 = math.log2(math.e) * HD ** (-0.5)
MESH = pl.DeviceIdType.MESH


def flipped(index, mask):
    out = index
    bit = 1
    while bit <= mask:
        if mask & bit:
            out = out + bit * (1 - 2 * lax.rem(index // bit, 2))
        bit *= 2
    return out


def kernel(
    nz,
    nt,
    seq_rep,
    local_heads,
    counts_ref,
    lengths_hbm,
    slot_seq_hbm,
    slot_block_hbm,
    residual_hbm,
    queries_hbm,
    new_kv_hbm,
    gain_hbm,
    cache_ref,
    weight_ref,
    stream_ref,
    factor_ref,
    lengths_ref,
    slot_seq_ref,
    slot_block_ref,
    residual_ref,
    queries_ref,
    new_kv_ref,
    gain_ref,
    wide_gain,
    cache_buf,
    weight_buf,
    bias_buf,
    row_buf,
    new_buf,
    q_all,
    pair_send,
    pair_recv,
    z_send,
    z_stat_send,
    z_part,
    z_stat,
    lhs_buf,
    proj_sum,
    proj_send,
    proj_recv,
    ss_send,
    ss_recv,
    input_sem,
    cache_sem,
    weight_sem,
    qz_recv,
    qt_recv,
    pair_sem,
    zp_recv,
    zs_recv,
    send_sem,
    rs_recv,
    sq_recv,
):
    z = lax.axis_index("kvb")
    t = lax.axis_index("tp")
    kv_local = max(1, local_heads // GROUP_HEADS)
    per_kv = local_heads // kv_local
    sub = per_kv * seq_rep
    rows = nz * sub
    tokens = cache_buf.shape[0]
    slots = slot_seq_ref.shape[1]
    width = stream_ref.shape[1]
    slow = nt // CORES
    QZ, QT, PAIR, ZP, ZS, RS, SQ = range(7)

    def z_peer(a):
        return flipped(z, a)

    def tp_peer(j):
        return flipped(t, j)

    far_first = sorted(range(1, nt), key=lambda j: (j < CORES, j))

    barrier = pltpu.get_barrier_semaphore()
    for a in range(1, nz):
        pl.semaphore_signal(barrier, inc=1, device_id={"kvb": z_peer(a)}, device_id_type=MESH)
    for j in range(1, nt):
        pl.semaphore_signal(barrier, inc=1, device_id={"tp": tp_peer(j)}, device_id_type=MESH)

    own = pl.ds(pl.multiple_of(t * width, LANES), width)
    inputs = [
        pltpu.make_async_copy(src, dst, input_sem.at[i])
        for i, (src, dst) in enumerate(
            (
                (queries_hbm, queries_ref),
                (slot_seq_hbm, slot_seq_ref),
                (slot_block_hbm, slot_block_ref),
                (new_kv_hbm, new_kv_ref),
                (residual_hbm.at[:, own], residual_ref),
                (gain_hbm, gain_ref),
                (lengths_hbm, lengths_ref),
            )
        )
    ]
    for copy in inputs:
        copy.start()
    cache_copy = pltpu.make_async_copy(cache_ref, cache_buf, cache_sem)
    cache_copy.start()
    inputs[0].wait()

    wide_q = queries_ref[...].astype(jnp.float32)
    for k in range(kv_local):
        for q in range(per_kv):
            head = k * per_kv + q
            row_buf[k, q * seq_rep : (q + 1) * seq_rep, :] = wide_q[:, head * HD : (head + 1) * HD]
    for k in range(kv_local):
        q_all[0, 0, k] = row_buf[k].astype(jnp.bfloat16)
    with jax.named_scope("barrier_wait"):
        pl.semaphore_wait(barrier, nz - 1 + nt - 1)

    def remote(src, dst, send, recv, target):
        pltpu.make_async_remote_copy(
            src_ref=src,
            dst_ref=dst,
            send_sem=send_sem.at[send],
            recv_sem=recv,
            device_id=target,
            device_id_type=MESH,
        ).start()

    def wait_bytes(ref, sem):
        pltpu.make_async_copy(ref, ref, sem).wait()

    for a in reversed(range(1, nz)):
        remote(q_all.at[0, 0], q_all.at[0, a], QZ, qz_recv.at[a - 1], {"kvb": z_peer(a)})

    def forward(a):
        for j in far_first:
            remote(q_all.at[0, a], q_all.at[j, a], QT, qt_recv.at[j - 1], {"tp": tp_peer(j)})

    forward(0)

    depth = weight_buf.shape[0] // kv_local
    pieces = 4
    for i in range(kv_local * pieces):
        part_rows = pl.ds(i * (depth // pieces), depth // pieces)
        pltpu.make_async_copy(
            weight_ref.at[part_rows, :], weight_buf.at[part_rows, :], weight_sem.at[i // pieces]
        ).start()
    for copy in inputs[1:]:
        copy.wait()

    row_id = lax.broadcasted_iota(jnp.int32, (rows, slots), 0)
    slot_id = lax.broadcasted_iota(jnp.int32, (rows, slots), 1)
    row_seq = jnp.zeros((rows, slots), jnp.int32)
    for a in range(nz):
        row_seq = jnp.where(row_id // sub == a, z_peer(a) * seq_rep, row_seq)
    row_seq += lax.rem(row_id, seq_rep)
    row_len = jnp.zeros((rows, slots), jnp.int32)
    for s in range(nz * seq_rep):
        row_len = jnp.where(row_seq == s, lengths_ref[s], row_len)
    held = (row_seq == slot_seq_ref[...]) & (slot_id < counts_ref[0])
    limit = jnp.where(held, jnp.clip(row_len - BLK * slot_block_ref[...], 0, BLK), 0)
    token_slot = lax.broadcasted_iota(jnp.int32, (slots, tokens), 1) // BLK
    spread = (token_slot == lax.broadcasted_iota(jnp.int32, (slots, tokens), 0)).astype(jnp.float32)
    reach = jnp.dot(
        limit.astype(jnp.float32).astype(jnp.bfloat16),
        spread.astype(jnp.bfloat16),
        preferred_element_type=jnp.float32,
    )
    offset = lax.rem(lax.broadcasted_iota(jnp.int32, (rows, tokens), 1), BLK).astype(jnp.float32)
    bias_buf[...] = jnp.where(offset < reach, 0.0, NEGATIVE)

    own_kv = t * local_heads // GROUP_HEADS
    fresh = []
    for k in range(kv_local):
        for part in range(2):
            at = pl.multiple_of((part * KVH + own_kv + k) * HD, LANES)
            piece = new_kv_ref[:, pl.ds(at, HD)].astype(jnp.float32)
            for q in range(per_kv):
                new_buf[k, part, q * seq_rep : (q + 1) * seq_rep, :] = piece
        fresh.append(jnp.sum(row_buf[k] * new_buf[k, 0], axis=1, keepdims=True) * TOKEN_LOG2)
    lhs_buf[...] = jnp.zeros_like(lhs_buf)
    gain = gain_ref[...].astype(jnp.float32).reshape(1, width)
    wide_gain[...] = jnp.broadcast_to(gain, wide_gain.shape)

    for a in range(1, nz):
        with jax.named_scope(f"q_z_wait{a}"):
            wait_bytes(q_all.at[0, a], qz_recv.at[a - 1])
        forward(a)

    with jax.named_scope("cache_wait"):
        cache_copy.wait()
    lane = lax.broadcasted_iota(jnp.int32, (rows, LANES), 1)
    kept = {}

    def attend(j, k):
        first_kv = tp_peer(j) * local_heads // GROUP_HEADS
        key_at = pl.multiple_of((first_kv + k) * HD, LANES)
        value_at = pl.multiple_of((KVH + first_kv + k) * HD, LANES)
        q_rows = q_all[j, :, k].reshape(rows, HD)
        scores = lax.dot_general(
            q_rows,
            cache_buf[:, pl.ds(key_at, HD)],
            (((1,), (1,)), ((), ())),
            preferred_element_type=jnp.float32,
        )
        scores = scores * TOKEN_LOG2 + bias_buf[...]
        peak = jnp.max(scores, axis=1, keepdims=True)
        weights = jnp.exp2(scores - jnp.maximum(peak, 0.1 * NEGATIVE))
        total = jnp.sum(weights, axis=1, keepdims=True)
        partial = jnp.dot(
            weights.astype(jnp.bfloat16),
            cache_buf[:, pl.ds(value_at, HD)],
            preferred_element_type=jnp.float32,
        )
        wide_peak = jnp.broadcast_to(peak, (rows, HD))
        wide_total = jnp.broadcast_to(total, (rows, HD))
        if j % CORES:
            kept[j // CORES, k] = (partial, wide_peak, wide_total)
            return
        for i, piece in enumerate((partial, wide_peak, wide_total)):
            pair_send[j // CORES, k, i] = piece
        remote(
            pair_send.at[j // CORES, k],
            pair_recv.at[j // CORES, k],
            PAIR,
            pair_sem.at[j // CORES * kv_local + k],
            {"tp": tp_peer(1)},
        )

    def join(jx, k):
        with jax.named_scope(f"pair_wait{jx}{k}"):
            wait_bytes(pair_recv.at[jx, k], pair_sem.at[jx * kv_local + k])
        partial, peak, total = kept.pop((jx, k))
        other, other_peak, other_total = (pair_recv[jx, k, i] for i in range(3))
        top = jnp.maximum(peak, other_peak)
        scale = jnp.exp2(peak - top)
        other_scale = jnp.exp2(other_peak - top)
        joined = scale * partial + other_scale * other
        z_send[jx, k] = joined.astype(jnp.bfloat16)
        total = scale * total + other_scale * other_total
        z_stat_send[jx, k] = jnp.where(lane == 0, top, total).T[:2]
        for a in reversed(range(nz)):
            target = {"kvb": z_peer(a), "tp": tp_peer(jx * CORES + 1)}
            remote(z_stat_send.at[jx, k], z_stat.at[k, jx, a], ZS, zs_recv.at[k], target)
            remote(
                z_send.at[jx, k, pl.ds(a * sub, sub)],
                z_part.at[k, jx, a],
                ZP,
                zp_recv.at[k],
                target,
            )

    for jx in range(slow):
        for jc in range(CORES):
            j = jx * CORES + jc
            if j > 0:
                with jax.named_scope(f"q_tp_wait{j}"):
                    wait_bytes(q_all.at[j], qt_recv.at[j - 1])
            for k in range(kv_local):
                attend(j, k)
                if jc and jx:
                    join(jx, k)
        if jx == 0:
            for k in range(kv_local):
                join(jx, k)

    def columns_of(pieces):
        height = -(-len(pieces) // 8) * 8
        index = lax.broadcasted_iota(jnp.int32, (height, rows), 0)
        tile = jnp.zeros((height, rows), jnp.float32)
        for i, piece in enumerate(pieces):
            tile = jnp.where(index == i, piece, tile)
        return tile.T

    sources = [(jx, a) for jx in range(slow) for a in range(nz)]
    for k in range(kv_local):
        with jax.named_scope(f"z_wait{k}"):
            wait_bytes(z_part.at[k], zp_recv.at[k])
            wait_bytes(z_stat.at[k], zs_recv.at[k])
        spread_stat = columns_of([z_stat[k, jx, a, i : i + 1, :] for jx, a in sources for i in range(2)])
        peaks, sums = (
            [
                spread_stat[a * sub : (a + 1) * sub, 2 * n + i : 2 * n + i + 1]
                for n, (_, a) in enumerate(sources)
            ]
            for i in range(2)
        )
        top = fresh[k]
        for piece in peaks:
            top = jnp.maximum(top, piece)
        denominator = jnp.exp2(fresh[k] - top)
        numerator = denominator * new_buf[k, 1]
        for n, (jx, a) in enumerate(sources):
            scale = jnp.exp2(peaks[n] - top)
            denominator += scale * sums[n]
            numerator += scale * z_part[k, jx, a].astype(jnp.float32)
        row_buf[k] = numerator / denominator
        for q in range(per_kv):
            lhs_buf[k, 0:seq_rep, q * HD : (q + 1) * HD] = row_buf[
                k, q * seq_rep : (q + 1) * seq_rep, :
            ]
        attended = lhs_buf[k].astype(jnp.bfloat16)
        with jax.named_scope(f"weight_wait{k}"):
            half = pl.ds(k * depth, depth)
            pltpu.make_async_copy(
                weight_ref.at[half, :], weight_buf.at[half, :], weight_sem.at[k]
            ).wait()
        for j in far_first + [0]:
            column = pl.ds(pl.multiple_of(tp_peer(j) * width, LANES), width)
            got = jnp.dot(
                attended,
                weight_buf[k * depth : (k + 1) * depth, column],
                preferred_element_type=jnp.float32,
            )[:seq_rep]
            if k > 0:
                got += proj_sum[j]
            if j == 0 or k < kv_local - 1:
                proj_sum[j] = got
                continue
            proj_send[j - 1] = got.astype(jnp.bfloat16)
            remote(proj_send.at[j - 1], proj_recv.at[j - 1], RS, rs_recv, {"tp": tp_peer(j)})
    summed = residual_ref[...].astype(jnp.float32) + proj_sum[0]
    for ref, send in (
        (q_all.at[0, pl.ds(1, nz - 1)], QZ),
        (q_all.at[pl.ds(1, nt - 1)], QT),
        (pair_send, PAIR),
        (z_part, ZP),
        (z_stat, ZS),
    ):
        wait_bytes(ref, send_sem.at[send])
    with jax.named_scope("sum_wait"):
        wait_bytes(proj_recv, rs_recv)
    for j in range(1, nt):
        summed += proj_recv[j - 1].astype(jnp.float32)
    stream = summed.astype(jnp.bfloat16)
    stream_wide = stream.astype(jnp.float32)
    stream_ref[...] = stream_wide
    square = jnp.sum(stream_wide * stream_wide, axis=1, keepdims=True)
    ss_send[...] = jnp.broadcast_to(square, ss_send.shape)
    for j in far_first:
        remote(ss_send, ss_recv.at[j - 1], SQ, sq_recv, {"tp": tp_peer(j)})
    with jax.named_scope("square_wait"):
        wait_bytes(ss_recv, sq_recv)
    for j in range(1, nt):
        square += ss_recv[j - 1][:, 0:1]
    mean_square = square * (1.0 / (width * nt))
    factor_ref[...] = lax.rsqrt(mean_square + EPSILON) * wide_gain[...]
    wait_bytes(proj_send, send_sem.at[RS])
    wait_bytes(ss_recv, send_sem.at[SQ])


def on_device(
    residual,
    queries,
    new_kv,
    kv_cache,
    lengths,
    slot_seq,
    slot_block,
    block_counts,
    out_weight,
    norm_gain,
):
    nt = lax.axis_size("tp")
    nz = lax.axis_size("kvb")
    seq_rep = residual.shape[0]
    local_heads = queries.shape[1] // HD
    kv_local = max(1, local_heads // GROUP_HEADS)
    sub = local_heads // kv_local * seq_rep
    rows = nz * sub
    slots = kv_cache.shape[0]
    tokens = slots * BLK
    width = norm_gain.shape[0]
    depth = out_weight.shape[0]
    slow = nt // CORES
    bf16, f32 = jnp.bfloat16, jnp.float32
    dma = pltpu.SemaphoreType.DMA
    smem = pl.BlockSpec(memory_space=pltpu.SMEM)
    vmem = pl.BlockSpec(memory_space=pltpu.VMEM)
    hbm = pl.BlockSpec(memory_space=pltpu.HBM)

    def body(*refs):
        kernel(nz, nt, seq_rep, local_heads, *refs)

    stream, factor = pl.pallas_call(
        body,
        out_shape=(
            jax.ShapeDtypeStruct((seq_rep, width), f32),
            jax.ShapeDtypeStruct((seq_rep, width), f32),
        ),
        in_specs=[smem] + [hbm] * 9,
        out_specs=(vmem, vmem),
        scratch_shapes=[
            pltpu.SMEM(lengths.shape, jnp.int32),
            pltpu.VMEM((1, slots), jnp.int32),
            pltpu.VMEM((1, slots), jnp.int32),
            pltpu.VMEM((seq_rep, width), bf16),
            pltpu.VMEM(queries.shape, bf16),
            pltpu.VMEM(new_kv.shape, bf16),
            pltpu.VMEM((width,), bf16),
            pltpu.VMEM((seq_rep, width), f32),
            pltpu.VMEM((tokens, kv_cache.shape[2]), bf16),
            pltpu.VMEM(out_weight.shape, bf16),
            pltpu.VMEM((rows, tokens), f32),
            pltpu.VMEM((kv_local, sub, HD), f32),
            pltpu.VMEM((kv_local, 2, sub, HD), f32),
            pltpu.VMEM((nt, nz, kv_local, sub, HD), bf16),
            pltpu.VMEM((slow, kv_local, 3, rows, HD), f32),
            pltpu.VMEM((slow, kv_local, 3, rows, HD), f32),
            pltpu.VMEM((slow, kv_local, rows, HD), bf16),
            pltpu.VMEM((slow, kv_local, 2, rows), f32),
            pltpu.VMEM((kv_local, slow, nz, sub, HD), bf16),
            pltpu.VMEM((kv_local, slow, nz, 2, rows), f32),
            pltpu.VMEM((kv_local, 16, depth // kv_local), f32),
            pltpu.VMEM((nt, seq_rep, width), f32),
            pltpu.VMEM((nt - 1, seq_rep, width), bf16),
            pltpu.VMEM((nt - 1, seq_rep, width), bf16),
            pltpu.VMEM((seq_rep, LANES), f32),
            pltpu.VMEM((nt - 1, seq_rep, LANES), f32),
            dma((7,)),
            dma,
            dma((kv_local,)),
            dma((nz - 1,)),
            dma((nt - 1,)),
            dma((slow * kv_local,)),
            dma((kv_local,)),
            dma((kv_local,)),
            dma((7,)),
            dma,
            dma,
        ],
        compiler_params=pltpu.CompilerParams(
            collective_id=0, has_side_effects=True, vmem_limit_bytes=46 * 1024 * 1024
        ),
    )(
        block_counts,
        *(
            pltpu.with_memory_space_constraint(operand, pltpu.HBM)
            for operand in (
                lengths,
                slot_seq.reshape(1, slots),
                slot_block.reshape(1, slots),
                residual,
                queries,
                new_kv,
                norm_gain,
                kv_cache.reshape(tokens, kv_cache.shape[2]),
                out_weight,
            )
        ),
    )
    return (stream.astype(bf16), (stream * factor).astype(bf16))


def solution(mesh):
    placed = (
        P(("groups", "kvb"), None),
        P(("groups", "kvb"), "tp"),
        P(("groups", "kvb"), None),
        P(("groups", "kvb", "tp"), None, None),
        P("groups"),
        P(("groups", "kvb", "tp")),
        P(("groups", "kvb", "tp")),
        P(("groups", "kvb", "tp")),
        P("tp", None),
        P("tp"),
    )
    return jax.shard_map(
        on_device,
        mesh=mesh,
        in_specs=placed,
        out_specs=(P(("groups", "kvb"), "tp"), P(("groups", "kvb"), "tp")),
        check_vma=False,
    )
```

```python
import math

import jax
import jax.numpy as jnp
from jax import lax
from jax.experimental import pallas as pl
from jax.experimental.pallas import tpu as pltpu
from jax.sharding import PartitionSpec as P

QH = 64
KVH = 8
HD = 128
BLK = 16
GROUP_HEADS = QH // KVH

NEGATIVE = -1e30
EPSILON = 1e-06
LANES = 128
CORES = 2
TOKEN_LOG2 = math.log2(math.e) * HD ** (-0.5)
MESH = pl.DeviceIdType.MESH


def flipped(index, mask):
    out = index
    bit = 1
    while bit <= mask:
        if mask & bit:
            out = out + bit * (1 - 2 * lax.rem(index // bit, 2))
        bit *= 2
    return out


def kernel(
    nz,
    nt,
    seq_rep,
    local_heads,
    counts_ref,
    lengths_hbm,
    slot_seq_hbm,
    slot_block_hbm,
    residual_hbm,
    queries_hbm,
    new_kv_hbm,
    gain_hbm,
    cache_ref,
    weight_ref,
    stream_ref,
    factor_ref,
    lengths_ref,
    slot_seq_ref,
    slot_block_ref,
    residual_ref,
    queries_ref,
    new_kv_ref,
    gain_ref,
    wide_gain,
    cache_buf,
    weight_buf,
    bias_buf,
    row_buf,
    new_buf,
    q_all,
    pair_send,
    pair_recv,
    z_send,
    z_stat_send,
    z_part,
    z_stat,
    lhs_buf,
    proj_sum,
    proj_send,
    proj_recv,
    ss_send,
    ss_recv,
    input_sem,
    cache_sem,
    weight_sem,
    q_recv,
    pair_sem,
    zp_recv,
    zs_recv,
    send_sem,
    rs_recv,
    sq_recv,
):
    z = lax.axis_index("kvb")
    t = lax.axis_index("tp")
    kv_local = max(1, local_heads // GROUP_HEADS)
    per_kv = local_heads // kv_local
    sub = per_kv * seq_rep
    rows = nz * sub
    tokens = cache_buf.shape[0]
    slots = slot_seq_ref.shape[1]
    width = stream_ref.shape[1]
    slow = nt // CORES
    QZ, QZ2, QT, PAIR, ZP, ZS, RS, SQ = range(8)

    def z_peer(a):
        return flipped(z, a)

    def tp_peer(j):
        return flipped(t, j)

    far_first = sorted(range(1, nt), key=lambda j: (j < CORES, j))

    barrier = pltpu.get_barrier_semaphore()
    chips = [(jx, a) for jx in range(slow) for a in reversed(range(nz)) if jx or a]

    def same_core(jx, a):
        return {"kvb": z_peer(a), "tp": tp_peer(jx * CORES)}

    for chip in chips:
        pl.semaphore_signal(barrier, inc=1, device_id=same_core(*chip), device_id_type=MESH)
    pl.semaphore_signal(barrier, inc=1, device_id={"tp": tp_peer(1)}, device_id_type=MESH)

    own = pl.ds(pl.multiple_of(t * width, LANES), width)
    inputs = [
        pltpu.make_async_copy(src, dst, input_sem.at[i])
        for i, (src, dst) in enumerate(
            (
                (queries_hbm, queries_ref),
                (slot_seq_hbm, slot_seq_ref),
                (slot_block_hbm, slot_block_ref),
                (new_kv_hbm, new_kv_ref),
                (residual_hbm.at[:, own], residual_ref),
                (gain_hbm, gain_ref),
                (lengths_hbm, lengths_ref),
            )
        )
    ]
    for copy in inputs:
        copy.start()
    cache_copy = pltpu.make_async_copy(cache_ref, cache_buf, cache_sem)
    cache_copy.start()
    inputs[0].wait()

    wide_q = queries_ref[...].astype(jnp.float32)
    for k in range(kv_local):
        for q in range(per_kv):
            head = k * per_kv + q
            row_buf[k, q * seq_rep : (q + 1) * seq_rep, :] = wide_q[:, head * HD : (head + 1) * HD]
    for k in range(kv_local):
        q_all[0, 0, k] = row_buf[k].astype(jnp.bfloat16)
    with jax.named_scope("barrier_wait"):
        pl.semaphore_wait(barrier, len(chips) + 1)

    def remote(src, dst, send, recv, target):
        pltpu.make_async_remote_copy(
            src_ref=src,
            dst_ref=dst,
            send_sem=send_sem.at[send],
            recv_sem=recv,
            device_id=target,
            device_id_type=MESH,
        ).start()

    def wait_bytes(ref, sem):
        pltpu.make_async_copy(ref, ref, sem).wait()

    for jx, a in chips:
        remote(q_all.at[0, 0], q_all.at[jx * CORES, a], QZ2 if jx else QZ, q_recv.at[jx * CORES], same_core(jx, a))

    def await_queries(jx):
        with jax.named_scope(f"q_wait{jx}"):
            landed = q_all.at[0, pl.ds(1, nz - 1)] if jx == 0 else q_all.at[jx * CORES]
            wait_bytes(landed, q_recv.at[jx * CORES])
        j = jx * CORES + 1
        remote(q_all.at[j - 1], q_all.at[j], QT, q_recv.at[j], {"tp": tp_peer(1)})

    depth = weight_buf.shape[0] // kv_local
    pieces = 4
    for i in range(kv_local * pieces):
        part_rows = pl.ds(i * (depth // pieces), depth // pieces)
        pltpu.make_async_copy(
            weight_ref.at[part_rows, :], weight_buf.at[part_rows, :], weight_sem.at[i // pieces]
        ).start()
    for copy in inputs[1:]:
        copy.wait()

    row_id = lax.broadcasted_iota(jnp.int32, (rows, slots), 0)
    slot_id = lax.broadcasted_iota(jnp.int32, (rows, slots), 1)
    row_seq = jnp.zeros((rows, slots), jnp.int32)
    for a in range(nz):
        row_seq = jnp.where(row_id // sub == a, z_peer(a) * seq_rep, row_seq)
    row_seq += lax.rem(row_id, seq_rep)
    row_len = jnp.zeros((rows, slots), jnp.int32)
    for s in range(nz * seq_rep):
        row_len = jnp.where(row_seq == s, lengths_ref[s], row_len)
    held = (row_seq == slot_seq_ref[...]) & (slot_id < counts_ref[0])
    limit = jnp.where(held, jnp.clip(row_len - BLK * slot_block_ref[...], 0, BLK), 0)
    token_slot = lax.broadcasted_iota(jnp.int32, (slots, tokens), 1) // BLK
    spread = (token_slot == lax.broadcasted_iota(jnp.int32, (slots, tokens), 0)).astype(jnp.float32)
    reach = jnp.dot(
        limit.astype(jnp.float32).astype(jnp.bfloat16),
        spread.astype(jnp.bfloat16),
        preferred_element_type=jnp.float32,
    )
    offset = lax.rem(lax.broadcasted_iota(jnp.int32, (rows, tokens), 1), BLK).astype(jnp.float32)
    bias_buf[...] = jnp.where(offset < reach, 0.0, NEGATIVE)

    own_kv = t * local_heads // GROUP_HEADS
    fresh = []
    for k in range(kv_local):
        for part in range(2):
            at = pl.multiple_of((part * KVH + own_kv + k) * HD, LANES)
            piece = new_kv_ref[:, pl.ds(at, HD)].astype(jnp.float32)
            for q in range(per_kv):
                new_buf[k, part, q * seq_rep : (q + 1) * seq_rep, :] = piece
        fresh.append(jnp.sum(row_buf[k] * new_buf[k, 0], axis=1, keepdims=True) * TOKEN_LOG2)
    lhs_buf[...] = jnp.zeros_like(lhs_buf)
    gain = gain_ref[...].astype(jnp.float32).reshape(1, width)
    wide_gain[...] = jnp.broadcast_to(gain, wide_gain.shape)

    await_queries(0)
    with jax.named_scope("cache_wait"):
        cache_copy.wait()
    lane = lax.broadcasted_iota(jnp.int32, (rows, LANES), 1)
    kept = {}

    def scores_of(j, k):
        first_kv = tp_peer(j) * local_heads // GROUP_HEADS
        key_at = pl.multiple_of((first_kv + k) * HD, LANES)
        q_rows = q_all[j, :, k].reshape(rows, HD)
        scores = lax.dot_general(
            q_rows,
            cache_buf[:, pl.ds(key_at, HD)],
            (((1,), (1,)), ((), ())),
            preferred_element_type=jnp.float32,
        )
        return scores * TOKEN_LOG2 + bias_buf[...]

    def attend(j, k, scores):
        first_kv = tp_peer(j) * local_heads // GROUP_HEADS
        value_at = pl.multiple_of((KVH + first_kv + k) * HD, LANES)
        peak = jnp.max(scores, axis=1, keepdims=True)
        weights = jnp.exp2(scores - jnp.maximum(peak, 0.1 * NEGATIVE))
        total = jnp.sum(weights, axis=1, keepdims=True)
        partial = jnp.dot(
            weights.astype(jnp.bfloat16),
            cache_buf[:, pl.ds(value_at, HD)],
            preferred_element_type=jnp.float32,
        )
        wide_peak = jnp.broadcast_to(peak, (rows, HD))
        wide_total = jnp.broadcast_to(total, (rows, HD))
        if j % CORES:
            kept[j // CORES, k] = (partial, wide_peak, wide_total)
            return
        for i, piece in enumerate((partial, wide_peak, wide_total)):
            pair_send[j // CORES, k, i] = piece
        remote(
            pair_send.at[j // CORES, k],
            pair_recv.at[j // CORES, k],
            PAIR,
            pair_sem.at[j // CORES * kv_local + k],
            {"tp": tp_peer(1)},
        )

    def join(jx, k):
        with jax.named_scope(f"pair_wait{jx}{k}"):
            wait_bytes(pair_recv.at[jx, k], pair_sem.at[jx * kv_local + k])
        partial, peak, total = kept.pop((jx, k))
        other, other_peak, other_total = (pair_recv[jx, k, i] for i in range(3))
        top = jnp.maximum(peak, other_peak)
        scale = jnp.exp2(peak - top)
        other_scale = jnp.exp2(other_peak - top)
        joined = scale * partial + other_scale * other
        z_send[jx, k] = joined.astype(jnp.bfloat16)
        total = scale * total + other_scale * other_total
        z_stat_send[jx, k] = jnp.where(lane == 0, top, total).T[:2]
        for a in reversed(range(nz)):
            target = {"kvb": z_peer(a), "tp": tp_peer(jx * CORES + 1)}
            remote(z_stat_send.at[jx, k], z_stat.at[k, jx, a], ZS, zs_recv.at[k], target)
            remote(
                z_send.at[jx, k, pl.ds(a * sub, sub)],
                z_part.at[k, jx, a],
                ZP,
                zp_recv.at[k],
                target,
            )

    for jx in range(slow):
        for jc in range(CORES):
            j = jx * CORES + jc
            if jc:
                with jax.named_scope(f"q_pair_wait{jx}"):
                    wait_bytes(q_all.at[j], q_recv.at[j])
            elif jx:
                await_queries(jx)
            scores = [scores_of(j, k) for k in range(kv_local)]
            for k in range(kv_local):
                attend(j, k, scores[k])
                if jc and jx:
                    join(jx, k)
        if jx == 0:
            for k in range(kv_local):
                join(jx, k)

    def columns_of(pieces):
        height = -(-len(pieces) // 8) * 8
        index = lax.broadcasted_iota(jnp.int32, (height, rows), 0)
        tile = jnp.zeros((height, rows), jnp.float32)
        for i, piece in enumerate(pieces):
            tile = jnp.where(index == i, piece, tile)
        return tile.T

    sources = [(jx, a) for jx in range(slow) for a in range(nz)]
    for k in range(kv_local):
        with jax.named_scope(f"z_wait{k}"):
            wait_bytes(z_part.at[k], zp_recv.at[k])
            wait_bytes(z_stat.at[k], zs_recv.at[k])
        spread_stat = columns_of([z_stat[k, jx, a, i : i + 1, :] for jx, a in sources for i in range(2)])
        peaks, sums = (
            [
                spread_stat[a * sub : (a + 1) * sub, 2 * n + i : 2 * n + i + 1]
                for n, (_, a) in enumerate(sources)
            ]
            for i in range(2)
        )
        top = fresh[k]
        for piece in peaks:
            top = jnp.maximum(top, piece)
        denominator = jnp.exp2(fresh[k] - top)
        numerator = denominator * new_buf[k, 1]
        for n, (jx, a) in enumerate(sources):
            scale = jnp.exp2(peaks[n] - top)
            denominator += scale * sums[n]
            numerator += scale * z_part[k, jx, a].astype(jnp.float32)
        row_buf[k] = numerator / denominator
        for q in range(per_kv):
            lhs_buf[k, 0:seq_rep, q * HD : (q + 1) * HD] = row_buf[
                k, q * seq_rep : (q + 1) * seq_rep, :
            ]
        attended = lhs_buf[k].astype(jnp.bfloat16)
        with jax.named_scope(f"weight_wait{k}"):
            half = pl.ds(k * depth, depth)
            pltpu.make_async_copy(
                weight_ref.at[half, :], weight_buf.at[half, :], weight_sem.at[k]
            ).wait()
        for j in far_first + [0]:
            column = pl.ds(pl.multiple_of(tp_peer(j) * width, LANES), width)
            got = jnp.dot(
                attended,
                weight_buf[k * depth : (k + 1) * depth, column],
                preferred_element_type=jnp.float32,
            )[:seq_rep]
            if k > 0:
                got += proj_sum[j]
            if j == 0 or k < kv_local - 1:
                proj_sum[j] = got
                continue
            proj_send[j - 1] = got.astype(jnp.bfloat16)
            remote(proj_send.at[j - 1], proj_recv.at[j - 1], RS, rs_recv, {"tp": tp_peer(j)})
    summed = residual_ref[...].astype(jnp.float32) + proj_sum[0]
    for ref, send in (
        (q_all.at[pl.ds(0, slow)], QT),
        (pair_send, PAIR),
        (z_part, ZP),
        (z_stat, ZS),
    ):
        wait_bytes(ref, send_sem.at[send])
    wait_bytes(q_all.at[0, pl.ds(1, nz - 1)], send_sem.at[QZ])
    if slow > 1:
        wait_bytes(q_all.at[pl.ds(1, slow - 1)], send_sem.at[QZ2])
    with jax.named_scope("sum_wait"):
        wait_bytes(proj_recv, rs_recv)
    for j in range(1, nt):
        summed += proj_recv[j - 1].astype(jnp.float32)
    stream = summed.astype(jnp.bfloat16)
    stream_wide = stream.astype(jnp.float32)
    stream_ref[...] = stream_wide
    square = jnp.sum(stream_wide * stream_wide, axis=1, keepdims=True)
    ss_send[...] = jnp.broadcast_to(square, ss_send.shape)
    for j in far_first:
        remote(ss_send, ss_recv.at[j - 1], SQ, sq_recv, {"tp": tp_peer(j)})
    with jax.named_scope("square_wait"):
        wait_bytes(ss_recv, sq_recv)
    for j in range(1, nt):
        square += ss_recv[j - 1][:, 0:1]
    mean_square = square * (1.0 / (width * nt))
    factor_ref[...] = lax.rsqrt(mean_square + EPSILON) * wide_gain[...]
    wait_bytes(proj_send, send_sem.at[RS])
    wait_bytes(ss_recv, send_sem.at[SQ])


def on_device(
    residual,
    queries,
    new_kv,
    kv_cache,
    lengths,
    slot_seq,
    slot_block,
    block_counts,
    out_weight,
    norm_gain,
):
    nt = lax.axis_size("tp")
    nz = lax.axis_size("kvb")
    seq_rep = residual.shape[0]
    local_heads = queries.shape[1] // HD
    kv_local = max(1, local_heads // GROUP_HEADS)
    sub = local_heads // kv_local * seq_rep
    rows = nz * sub
    slots = kv_cache.shape[0]
    tokens = slots * BLK
    width = norm_gain.shape[0]
    depth = out_weight.shape[0]
    slow = nt // CORES
    bf16, f32 = jnp.bfloat16, jnp.float32
    dma = pltpu.SemaphoreType.DMA
    smem = pl.BlockSpec(memory_space=pltpu.SMEM)
    vmem = pl.BlockSpec(memory_space=pltpu.VMEM)
    hbm = pl.BlockSpec(memory_space=pltpu.HBM)

    def body(*refs):
        kernel(nz, nt, seq_rep, local_heads, *refs)

    stream, factor = pl.pallas_call(
        body,
        out_shape=(
            jax.ShapeDtypeStruct((seq_rep, width), f32),
            jax.ShapeDtypeStruct((seq_rep, width), f32),
        ),
        in_specs=[smem] + [hbm] * 9,
        out_specs=(vmem, vmem),
        scratch_shapes=[
            pltpu.SMEM(lengths.shape, jnp.int32),
            pltpu.VMEM((1, slots), jnp.int32),
            pltpu.VMEM((1, slots), jnp.int32),
            pltpu.VMEM((seq_rep, width), bf16),
            pltpu.VMEM(queries.shape, bf16),
            pltpu.VMEM(new_kv.shape, bf16),
            pltpu.VMEM((width,), bf16),
            pltpu.VMEM((seq_rep, width), f32),
            pltpu.VMEM((tokens, kv_cache.shape[2]), bf16),
            pltpu.VMEM(out_weight.shape, bf16),
            pltpu.VMEM((rows, tokens), f32),
            pltpu.VMEM((kv_local, sub, HD), f32),
            pltpu.VMEM((kv_local, 2, sub, HD), f32),
            pltpu.VMEM((nt, nz, kv_local, sub, HD), bf16),
            pltpu.VMEM((slow, kv_local, 3, rows, HD), f32),
            pltpu.VMEM((slow, kv_local, 3, rows, HD), f32),
            pltpu.VMEM((slow, kv_local, rows, HD), bf16),
            pltpu.VMEM((slow, kv_local, 2, rows), f32),
            pltpu.VMEM((kv_local, slow, nz, sub, HD), bf16),
            pltpu.VMEM((kv_local, slow, nz, 2, rows), f32),
            pltpu.VMEM((kv_local, 16, depth // kv_local), f32),
            pltpu.VMEM((nt, seq_rep, width), f32),
            pltpu.VMEM((nt - 1, seq_rep, width), bf16),
            pltpu.VMEM((nt - 1, seq_rep, width), bf16),
            pltpu.VMEM((seq_rep, LANES), f32),
            pltpu.VMEM((nt - 1, seq_rep, LANES), f32),
            dma((7,)),
            dma,
            dma((kv_local,)),
            dma((nt,)),
            dma((slow * kv_local,)),
            dma((kv_local,)),
            dma((kv_local,)),
            dma((8,)),
            dma,
            dma,
        ],
        compiler_params=pltpu.CompilerParams(
            collective_id=0, has_side_effects=True, vmem_limit_bytes=46 * 1024 * 1024
        ),
    )(
        block_counts,
        *(
            pltpu.with_memory_space_constraint(operand, pltpu.HBM)
            for operand in (
                lengths,
                slot_seq.reshape(1, slots),
                slot_block.reshape(1, slots),
                residual,
                queries,
                new_kv,
                norm_gain,
                kv_cache.reshape(tokens, kv_cache.shape[2]),
                out_weight,
            )
        ),
    )
    return (stream.astype(bf16), (stream * factor).astype(bf16))


def solution(mesh):
    placed = (
        P(("groups", "kvb"), None),
        P(("groups", "kvb"), "tp"),
        P(("groups", "kvb"), None),
        P(("groups", "kvb", "tp"), None, None),
        P("groups"),
        P(("groups", "kvb", "tp")),
        P(("groups", "kvb", "tp")),
        P(("groups", "kvb", "tp")),
        P("tp", None),
        P("tp"),
    )
    return jax.shard_map(
        on_device,
        mesh=mesh,
        in_specs=placed,
        out_specs=(P(("groups", "kvb"), "tp"), P(("groups", "kvb"), "tp")),
        check_vma=False,
    )
```

```python
import math

import jax
import jax.numpy as jnp
from jax import lax
from jax.experimental import pallas as pl
from jax.experimental.pallas import tpu as pltpu
from jax.sharding import PartitionSpec as P

QH = 64
KVH = 8
HD = 128
BLK = 16
GROUP_HEADS = QH // KVH

NEGATIVE = -1e30
EPSILON = 1e-06
LANES = 128
CORES = 2
TILE = 8
TOKEN_LOG2 = math.log2(math.e) * HD ** (-0.5)
MESH = pl.DeviceIdType.MESH


def flipped(index, mask):
    out = index
    bit = 1
    while bit <= mask:
        if mask & bit:
            out = out + bit * (1 - 2 * lax.rem(index // bit, 2))
        bit *= 2
    return out


def kernel(
    nz,
    nt,
    seq_rep,
    local_heads,
    counts_ref,
    lengths_hbm,
    slot_seq_hbm,
    slot_block_hbm,
    residual_hbm,
    queries_hbm,
    new_kv_hbm,
    gain_hbm,
    cache_ref,
    weight_ref,
    stream_ref,
    factor_ref,
    lengths_ref,
    slot_seq_ref,
    slot_block_ref,
    residual_ref,
    queries_ref,
    new_kv_ref,
    gain_ref,
    wide_gain,
    cache_buf,
    weight_buf,
    bias_buf,
    row_buf,
    new_buf,
    q_all,
    pair_send,
    pair_recv,
    z_send,
    z_stat_send,
    z_part,
    z_stat,
    fresh_buf,
    fresh_values,
    chosen_buf,
    proj_sum,
    proj_send,
    proj_recv,
    ss_send,
    ss_recv,
    input_sem,
    cache_sem,
    weight_sem,
    q_recv,
    pair_sem,
    zp_recv,
    zs_recv,
    send_sem,
    rs_recv,
    sq_recv,
):
    z = lax.axis_index("kvb")
    t = lax.axis_index("tp")
    kv_local = max(1, local_heads // GROUP_HEADS)
    per_kv = local_heads // kv_local
    sub = per_kv * seq_rep
    rows = nz * sub
    tokens = cache_buf.shape[0]
    slots = slot_seq_ref.shape[1]
    width = stream_ref.shape[1]
    slow = nt // CORES
    QZ, QZ2, QT, PAIR, ZP, ZS, RS, SQ = range(8)

    def z_peer(a):
        return flipped(z, a)

    def tp_peer(j):
        return flipped(t, j)

    far_first = sorted(range(1, nt), key=lambda j: (j < CORES, j))

    barrier = pltpu.get_barrier_semaphore()
    chips = [(jx, a) for jx in range(slow) for a in reversed(range(nz)) if jx or a]

    def same_core(jx, a):
        return {"kvb": z_peer(a), "tp": tp_peer(jx * CORES)}

    for chip in chips:
        pl.semaphore_signal(barrier, inc=1, device_id=same_core(*chip), device_id_type=MESH)
    pl.semaphore_signal(barrier, inc=1, device_id={"tp": tp_peer(1)}, device_id_type=MESH)

    own = pl.ds(pl.multiple_of(t * width, LANES), width)
    inputs = [
        pltpu.make_async_copy(src, dst, input_sem.at[i])
        for i, (src, dst) in enumerate(
            (
                (queries_hbm, queries_ref),
                (slot_seq_hbm, slot_seq_ref),
                (slot_block_hbm, slot_block_ref),
                (new_kv_hbm, new_kv_ref),
                (residual_hbm.at[:, own], residual_ref),
                (gain_hbm, gain_ref),
                (lengths_hbm, lengths_ref),
            )
        )
    ]
    for copy in inputs:
        copy.start()
    cache_copy = pltpu.make_async_copy(cache_ref, cache_buf, cache_sem)
    cache_copy.start()
    inputs[0].wait()
    depth = weight_buf.shape[0] // kv_local
    pieces = 4
    for i in range(kv_local * pieces):
        part_rows = pl.ds(i * (depth // pieces), depth // pieces)
        pltpu.make_async_copy(
            weight_ref.at[part_rows, :], weight_buf.at[part_rows, :], weight_sem.at[i // pieces]
        ).start()

    wide_q = queries_ref[...].astype(jnp.float32)
    for k in range(kv_local):
        for q in range(per_kv):
            head = k * per_kv + q
            row_buf[k, q * seq_rep : (q + 1) * seq_rep, :] = wide_q[:, head * HD : (head + 1) * HD]
    for k in range(kv_local):
        q_all[0, 0, k] = row_buf[k].astype(jnp.bfloat16)
    with jax.named_scope("barrier_wait"):
        pl.semaphore_wait(barrier, len(chips) + 1)

    def remote(src, dst, send, recv, target):
        pltpu.make_async_remote_copy(
            src_ref=src,
            dst_ref=dst,
            send_sem=send_sem.at[send],
            recv_sem=recv,
            device_id=target,
            device_id_type=MESH,
        ).start()

    def wait_bytes(ref, sem):
        pltpu.make_async_copy(ref, ref, sem).wait()

    for jx, a in chips:
        remote(q_all.at[0, 0], q_all.at[jx * CORES, a], QZ2 if jx else QZ, q_recv.at[jx * CORES], same_core(jx, a))

    def await_queries(jx):
        with jax.named_scope(f"q_wait{jx}"):
            landed = q_all.at[0, pl.ds(1, nz - 1)] if jx == 0 else q_all.at[jx * CORES]
            wait_bytes(landed, q_recv.at[jx * CORES])
        j = jx * CORES + 1
        remote(q_all.at[j - 1], q_all.at[j], QT, q_recv.at[j], {"tp": tp_peer(1)})

    for copy in inputs[1:]:
        copy.wait()

    row_id = lax.broadcasted_iota(jnp.int32, (rows, slots), 0)
    slot_id = lax.broadcasted_iota(jnp.int32, (rows, slots), 1)
    row_seq = jnp.zeros((rows, slots), jnp.int32)
    for a in range(nz):
        row_seq = jnp.where(row_id // sub == a, z_peer(a) * seq_rep, row_seq)
    row_seq += lax.rem(row_id, seq_rep)
    row_len = jnp.zeros((rows, slots), jnp.int32)
    for s in range(nz * seq_rep):
        row_len = jnp.where(row_seq == s, lengths_ref[s], row_len)
    held = (row_seq == slot_seq_ref[...]) & (slot_id < counts_ref[0])
    limit = jnp.where(held, jnp.clip(row_len - BLK * slot_block_ref[...], 0, BLK), 0)
    token_slot = lax.broadcasted_iota(jnp.int32, (slots, tokens), 1) // BLK
    spread = (token_slot == lax.broadcasted_iota(jnp.int32, (slots, tokens), 0)).astype(jnp.float32)
    reach = jnp.dot(
        limit.astype(jnp.float32).astype(jnp.bfloat16),
        spread.astype(jnp.bfloat16),
        preferred_element_type=jnp.float32,
    )
    offset = lax.rem(lax.broadcasted_iota(jnp.int32, (rows, tokens), 1), BLK).astype(jnp.float32)
    bias_buf[...] = jnp.where(offset < reach, 0.0, NEGATIVE)

    own_kv = t * local_heads // GROUP_HEADS
    for k in range(kv_local):
        for part in range(2):
            at = pl.multiple_of((part * KVH + own_kv + k) * HD, LANES)
            piece = new_kv_ref[:, pl.ds(at, HD)].astype(jnp.float32)
            for q in range(per_kv):
                new_buf[k, part, q * seq_rep : (q + 1) * seq_rep, :] = piece
        fresh = jnp.sum(row_buf[k] * new_buf[k, 0], axis=1, keepdims=True) * TOKEN_LOG2
        fresh = jnp.concatenate([fresh] * nz, axis=0)
        fresh_buf[k] = jnp.broadcast_to(fresh, (rows, LANES)).T[:8]
        blank = jnp.zeros((rows - sub, HD), jnp.float32)
        fresh_values[k] = jnp.concatenate([new_buf[k, 1], blank], axis=0).astype(jnp.bfloat16)
    out_row = lax.broadcasted_iota(jnp.int32, chosen_buf.shape, 0)
    in_row = lax.rem(lax.broadcasted_iota(jnp.int32, chosen_buf.shape, 1), sub)
    out_seq = lax.rem(out_row, TILE)
    chosen = (out_seq < seq_rep) & (in_row == out_row // TILE * seq_rep + out_seq)
    chosen_buf[...] = chosen.astype(jnp.float32)
    gain = gain_ref[...].astype(jnp.float32).reshape(1, width)
    wide_gain[...] = jnp.broadcast_to(gain, wide_gain.shape)

    await_queries(0)
    with jax.named_scope("cache_wait"):
        cache_copy.wait()
    lane = lax.broadcasted_iota(jnp.int32, (rows, LANES), 1)
    kept = {}

    def scores_of(j, k):
        first_kv = tp_peer(j) * local_heads // GROUP_HEADS
        key_at = pl.multiple_of((first_kv + k) * HD, LANES)
        q_rows = q_all[j, :, k].reshape(rows, HD)
        scores = lax.dot_general(
            q_rows,
            cache_buf[:, pl.ds(key_at, HD)],
            (((1,), (1,)), ((), ())),
            preferred_element_type=jnp.float32,
        )
        return scores * TOKEN_LOG2 + bias_buf[...]

    def attend(j, k, scores):
        first_kv = tp_peer(j) * local_heads // GROUP_HEADS
        value_at = pl.multiple_of((KVH + first_kv + k) * HD, LANES)
        peak = jnp.max(scores, axis=1, keepdims=True)
        weights = jnp.exp2(scores - jnp.maximum(peak, 0.1 * NEGATIVE))
        total = jnp.sum(weights, axis=1, keepdims=True)
        partial = jnp.dot(
            weights.astype(jnp.bfloat16),
            cache_buf[:, pl.ds(value_at, HD)],
            preferred_element_type=jnp.float32,
        )
        wide_peak = jnp.broadcast_to(peak, (rows, HD))
        wide_total = jnp.broadcast_to(total, (rows, HD))
        if j % CORES:
            kept[j // CORES, k] = (partial, wide_peak, wide_total)
            return
        for i, piece in enumerate((partial, wide_peak, wide_total)):
            pair_send[j // CORES, k, i] = piece
        remote(
            pair_send.at[j // CORES, k],
            pair_recv.at[j // CORES, k],
            PAIR,
            pair_sem.at[j // CORES * kv_local + k],
            {"tp": tp_peer(1)},
        )

    def join(jx, k):
        with jax.named_scope(f"pair_wait{jx}{k}"):
            wait_bytes(pair_recv.at[jx, k], pair_sem.at[jx * kv_local + k])
        partial, peak, total = kept.pop((jx, k))
        other, other_peak, other_total = (pair_recv[jx, k, i] for i in range(3))
        top = jnp.maximum(peak, other_peak)
        scale = jnp.exp2(peak - top)
        other_scale = jnp.exp2(other_peak - top)
        joined = scale * partial + other_scale * other
        z_send[jx, k] = joined.astype(jnp.bfloat16)
        total = scale * total + other_scale * other_total
        z_stat_send[jx, k] = jnp.where(lane == 0, top, total).T[:2]
        for a in reversed(range(nz)):
            target = {"kvb": z_peer(a), "tp": tp_peer(jx * CORES + 1)}
            remote(z_stat_send.at[jx, k], z_stat.at[k, jx, a], ZS, zs_recv.at[k], target)
            remote(
                z_send.at[jx, k, pl.ds(a * sub, sub)],
                z_part.at[k, jx, a],
                ZP,
                zp_recv.at[k],
                target,
            )

    for jx in range(slow):
        for jc in range(CORES):
            j = jx * CORES + jc
            if jc:
                with jax.named_scope(f"q_pair_wait{jx}"):
                    wait_bytes(q_all.at[j], q_recv.at[j])
            elif jx:
                await_queries(jx)
            scores = [scores_of(j, k) for k in range(kv_local)]
            for k in range(kv_local):
                attend(j, k, scores[k])
                if jc and jx:
                    join(jx, k)
        if jx == 0:
            for k in range(kv_local):
                join(jx, k)

    def over_sources(row, pick):
        turned = [pltpu.roll(row, a * sub, 1) for a in range(1, nz)]
        for other in turned:
            row = pick(row, other)
        return row

    def attended_of(k):
        with jax.named_scope(f"z_wait{k}"):
            wait_bytes(z_stat.at[k], zs_recv.at[k])
            wait_bytes(z_part.at[k], zp_recv.at[k])
        peaks, sums = ([stat_row(k, jx, i) for jx in range(slow)] for i in range(2))
        own_score = fresh_buf[k]
        top = own_score
        for piece in peaks:
            top = jnp.maximum(top, piece)
        top = over_sources(top, jnp.maximum)
        scales = [jnp.exp2(piece - top) for piece in peaks]
        denominator = sum(scale * piece for scale, piece in zip(scales, sums))
        own_scale = jnp.exp2(own_score - top)
        inverse = 1.0 / (over_sources(denominator, jnp.add) + own_scale)
        total = jnp.zeros((per_kv * TILE, HD), jnp.float32)
        blocks = [z_part[k, jx].reshape(rows, HD) for jx in range(slow)] + [fresh_values[k]]
        factors = [scale * inverse for scale in scales] + [own_scale * inverse]
        for n in range(0, slow + 1, 2):
            wide = jnp.concatenate(
                [
                    chosen_buf[...] * jnp.broadcast_to(factor[0:1], chosen_buf.shape)
                    for factor in factors[n : n + 2]
                ],
                axis=1,
            )
            high = wide.astype(jnp.bfloat16)
            low = (wide - high.astype(jnp.float32)).astype(jnp.bfloat16)
            block = jnp.concatenate(blocks[n : n + 2], axis=0)
            total += jnp.dot(high, block, preferred_element_type=jnp.float32)
            total += jnp.dot(low, block, preferred_element_type=jnp.float32)
        line = jnp.concatenate([total[q * TILE : (q + 1) * TILE] for q in range(per_kv)], axis=1)
        return jnp.concatenate([line, jnp.zeros_like(line)], axis=0).astype(jnp.bfloat16)

    def stat_row(k, jx, i):
        row = jnp.zeros((8, rows), jnp.float32)
        row_lane = lax.broadcasted_iota(jnp.int32, (8, rows), 1) // sub
        for a in range(nz):
            row = jnp.where(row_lane == a, z_stat[k, jx, a, i : i + 1, :], row)
        return row

    def project(k, j):
        column = pl.ds(pl.multiple_of(tp_peer(j) * width, LANES), width)
        return jnp.dot(
            attended[k],
            weight_buf[k * depth : (k + 1) * depth, column],
            preferred_element_type=jnp.float32,
        )[:seq_rep]

    def send_block(j):
        proj_send[j - 1] = proj_sum[j].astype(jnp.bfloat16)
        remote(proj_send.at[j - 1], proj_recv.at[j - 1], RS, rs_recv, {"tp": tp_peer(j)})

    for k in range(kv_local):
        with jax.named_scope(f"weight_wait{k}"):
            half = pl.ds(k * depth, depth)
            pltpu.make_async_copy(
                weight_ref.at[half, :], weight_buf.at[half, :], weight_sem.at[k]
            ).wait()
    attended = [attended_of(k) for k in range(kv_local)]
    for j in far_first + [0]:
        proj_sum[j] = sum(project(k, j) for k in range(kv_local))
        if j > 0:
            send_block(j)
    summed = residual_ref[...].astype(jnp.float32) + proj_sum[0]
    for ref, send in (
        (q_all.at[pl.ds(0, slow)], QT),
        (pair_send, PAIR),
        (z_part, ZP),
        (z_stat, ZS),
    ):
        wait_bytes(ref, send_sem.at[send])
    wait_bytes(q_all.at[0, pl.ds(1, nz - 1)], send_sem.at[QZ])
    if slow > 1:
        wait_bytes(q_all.at[pl.ds(1, slow - 1)], send_sem.at[QZ2])
    with jax.named_scope("sum_wait"):
        wait_bytes(proj_recv, rs_recv)
    for j in range(1, nt):
        summed += proj_recv[j - 1].astype(jnp.float32)
    stream = summed.astype(jnp.bfloat16)
    stream_wide = stream.astype(jnp.float32)
    stream_ref[...] = stream_wide
    square = jnp.sum(stream_wide * stream_wide, axis=1, keepdims=True)
    ss_send[...] = jnp.broadcast_to(square, ss_send.shape)
    for j in far_first:
        remote(ss_send, ss_recv.at[j - 1], SQ, sq_recv, {"tp": tp_peer(j)})
    with jax.named_scope("square_wait"):
        wait_bytes(ss_recv, sq_recv)
    for j in range(1, nt):
        square += ss_recv[j - 1][:, 0:1]
    mean_square = square * (1.0 / (width * nt))
    factor_ref[...] = lax.rsqrt(mean_square + EPSILON) * wide_gain[...]
    wait_bytes(proj_send, send_sem.at[RS])
    wait_bytes(ss_recv, send_sem.at[SQ])


def on_device(
    residual,
    queries,
    new_kv,
    kv_cache,
    lengths,
    slot_seq,
    slot_block,
    block_counts,
    out_weight,
    norm_gain,
):
    nt = lax.axis_size("tp")
    nz = lax.axis_size("kvb")
    seq_rep = residual.shape[0]
    local_heads = queries.shape[1] // HD
    kv_local = max(1, local_heads // GROUP_HEADS)
    sub = local_heads // kv_local * seq_rep
    rows = nz * sub
    slots = kv_cache.shape[0]
    tokens = slots * BLK
    width = norm_gain.shape[0]
    depth = out_weight.shape[0]
    slow = nt // CORES
    bf16, f32 = jnp.bfloat16, jnp.float32
    dma = pltpu.SemaphoreType.DMA
    smem = pl.BlockSpec(memory_space=pltpu.SMEM)
    vmem = pl.BlockSpec(memory_space=pltpu.VMEM)
    hbm = pl.BlockSpec(memory_space=pltpu.HBM)

    def body(*refs):
        kernel(nz, nt, seq_rep, local_heads, *refs)

    stream, factor = pl.pallas_call(
        body,
        out_shape=(
            jax.ShapeDtypeStruct((seq_rep, width), f32),
            jax.ShapeDtypeStruct((seq_rep, width), f32),
        ),
        in_specs=[smem] + [hbm] * 9,
        out_specs=(vmem, vmem),
        scratch_shapes=[
            pltpu.SMEM(lengths.shape, jnp.int32),
            pltpu.VMEM((1, slots), jnp.int32),
            pltpu.VMEM((1, slots), jnp.int32),
            pltpu.VMEM((seq_rep, width), bf16),
            pltpu.VMEM(queries.shape, bf16),
            pltpu.VMEM(new_kv.shape, bf16),
            pltpu.VMEM((width,), bf16),
            pltpu.VMEM((seq_rep, width), f32),
            pltpu.VMEM((tokens, kv_cache.shape[2]), bf16),
            pltpu.VMEM(out_weight.shape, bf16),
            pltpu.VMEM((rows, tokens), f32),
            pltpu.VMEM((kv_local, sub, HD), f32),
            pltpu.VMEM((kv_local, 2, sub, HD), f32),
            pltpu.VMEM((nt, nz, kv_local, sub, HD), bf16),
            pltpu.VMEM((slow, kv_local, 3, rows, HD), f32),
            pltpu.VMEM((slow, kv_local, 3, rows, HD), f32),
            pltpu.VMEM((slow, kv_local, rows, HD), bf16),
            pltpu.VMEM((slow, kv_local, 2, rows), f32),
            pltpu.VMEM((kv_local, slow, nz, sub, HD), bf16),
            pltpu.VMEM((kv_local, slow, nz, 2, rows), f32),
            pltpu.VMEM((kv_local, 8, rows), f32),
            pltpu.VMEM((kv_local, rows, HD), bf16),
            pltpu.VMEM((sub // seq_rep * TILE, rows), f32),
            pltpu.VMEM((nt, seq_rep, width), f32),
            pltpu.VMEM((nt - 1, seq_rep, width), bf16),
            pltpu.VMEM((nt - 1, seq_rep, width), bf16),
            pltpu.VMEM((seq_rep, LANES), f32),
            pltpu.VMEM((nt - 1, seq_rep, LANES), f32),
            dma((7,)),
            dma,
            dma((kv_local,)),
            dma((nt,)),
            dma((slow * kv_local,)),
            dma((kv_local,)),
            dma((kv_local,)),
            dma((8,)),
            dma,
            dma,
        ],
        compiler_params=pltpu.CompilerParams(
            collective_id=0, has_side_effects=True, vmem_limit_bytes=46 * 1024 * 1024
        ),
    )(
        block_counts,
        *(
            pltpu.with_memory_space_constraint(operand, pltpu.HBM)
            for operand in (
                lengths,
                slot_seq.reshape(1, slots),
                slot_block.reshape(1, slots),
                residual,
                queries,
                new_kv,
                norm_gain,
                kv_cache.reshape(tokens, kv_cache.shape[2]),
                out_weight,
            )
        ),
    )
    return (stream.astype(bf16), (stream * factor).astype(bf16))


def solution(mesh):
    placed = (
        P(("groups", "kvb"), None),
        P(("groups", "kvb"), "tp"),
        P(("groups", "kvb"), None),
        P(("groups", "kvb", "tp"), None, None),
        P("groups"),
        P(("groups", "kvb", "tp")),
        P(("groups", "kvb", "tp")),
        P(("groups", "kvb", "tp")),
        P("tp", None),
        P("tp"),
    )
    return jax.shard_map(
        on_device,
        mesh=mesh,
        in_specs=placed,
        out_specs=(P(("groups", "kvb"), "tp"), P(("groups", "kvb"), "tp")),
        check_vma=False,
    )
```
